32 devices in a mesh: dp: 4 (over x, core), center: 8 (over z, y).
Axes of the slice: x: 2, y: 2, z: 4, core: 2. Of those that a mesh axis runs over, the one named last changes fastest.
Arguments:
- features: bfloat16 [4096, 1024], P('dp'), may hold values from -6 to 6
- centers: bfloat16 [4096, 1024], P('center'), may hold values from -6 to 6
- targets: bfloat16 [4096, 256], P('dp'), may hold values from -6 to 6
Outputs:
- coef: float32 [4096, 256], P('center')
- residual: float32 [4096, 256], P('center')
The draws below stay inside these ranges and needn't reach their ends.
All inputs are finite; a program needn't handle non-finite values.
Results may differ from the reference program's by a relative error of at most 0.024.
Values may be sent and summed in bfloat16 or wider, within the bound.
No kernel may reach another device: no remote copies, remote signals or barrier semaphores. Data moves between devices by JAX's collectives and lax.ppermute only.
A program may use at most 64 MiB of HBM per device.

```python
import math
import jax
import jax.numpy as jnp
from jax import lax

D = 1024
TARGETS = 256
N_DEV = 1024
ITERS = 2
EXAMPLES = 4096
CENTERS = 4096


def level_of(stream_key, shape, cuts, low, top_value):
    loudness = 1.0
    for axis_at, blocks in cuts:
        heights = jax.random.uniform(jax.random.fold_in(jax.random.fold_in(stream_key, 6), axis_at), (blocks,), jnp.float32, low / len(cuts), top_value / len(cuts))
        loudness = loudness * jnp.repeat(jnp.exp(heights), shape[axis_at] // blocks).reshape((-1,) + (1,) * (len(shape) - 1 - axis_at))
    return loudness


def noise(rng, extent, width, bound, shards=(), kind=jnp.bfloat16):
    entries = width * jax.random.normal(rng, extent, jnp.float32)
    if shards:
        entries = entries * level_of(rng, extent, shards, -0.22, 0.18)
    return jnp.clip(entries, -bound, bound).astype(kind)


def setup_inputs(seed: int = 0) -> dict:
    arg_keys = jax.random.split(jax.random.key(seed), 4)
    return {
        "features": noise(arg_keys[0], (EXAMPLES, D), 1.0, 6.0, ((0, 4),)),
        "centers": noise(arg_keys[1], (CENTERS, D), 1.0, 6.0, ((0, 8),)),
        "targets": noise(arg_keys[2], (EXAMPLES, TARGETS), 1.0, 6.0, ((0, 4),)),
    }


def kernel_block(rows, centers):
    scores = lax.dot_general(rows, centers, (((1,), (1,)), ((), ())), preferred_element_type=jnp.float32)
    lifted = 1.0 + 0.5 / math.sqrt(rows.shape[1]) * scores
    return (lifted * lifted * lifted).astype(jnp.bfloat16)

def transposed_dot(kernel, values):
    return lax.dot_general(kernel, values, (((0,), (0,)), ((), ())), preferred_element_type=jnp.float32)

def right_hand(features, centers, targets):
    blocks = features.shape[0] // N_DEV

    def one_block(total, block_index):
        rows = lax.dynamic_slice_in_dim(features, block_index * N_DEV, N_DEV, 0)
        values = lax.dynamic_slice_in_dim(targets, block_index * N_DEV, N_DEV, 0)
        kernel = kernel_block(rows, centers)
        return (total + transposed_dot(kernel, values), None)
    start = jnp.zeros((centers.shape[0], targets.shape[1]), jnp.float32)
    total, unused = lax.scan(one_block, start, jnp.arange(blocks, dtype=jnp.int32))
    return total / math.sqrt(features.shape[0])

def apply_operator(features, centers, direction):
    blocks = features.shape[0] // N_DEV
    low_dir = direction.astype(jnp.bfloat16)

    def one_block(total, block_index):
        rows = lax.dynamic_slice_in_dim(features, block_index * N_DEV, N_DEV, 0)
        kernel = kernel_block(rows, centers)
        predicted = jnp.dot(kernel, low_dir, preferred_element_type=jnp.float32).astype(jnp.bfloat16)
        return (total + transposed_dot(kernel, predicted), None)
    start = jnp.zeros(direction.shape, jnp.float32)
    total, unused = lax.scan(one_block, start, jnp.arange(blocks, dtype=jnp.int32))
    return total / features.shape[0] + 0.5 * direction

def reference(features, centers, targets):
    right_side = right_hand(features, centers, targets)
    coef = jnp.zeros_like(right_side)
    residual = right_side
    direction = right_side
    norm_now = lax.optimization_barrier(jnp.sum(residual * residual, axis=0))
    for turn in range(ITERS):
        image = apply_operator(features, centers, direction)
        curvature = lax.optimization_barrier(jnp.sum(direction * image, axis=0))
        step_size = norm_now / (curvature + 1e-06)
        coef = coef + step_size * direction
        residual = residual - step_size * image
        if turn + 1 < ITERS:
            norm_next = lax.optimization_barrier(jnp.sum(residual * residual, axis=0))
            direction = residual + norm_next / (norm_now + 1e-06) * direction
            norm_now = norm_next
    return (coef, residual)
```

```python
import functools
import math

import jax
import jax.numpy as jnp
from jax import lax
from jax.experimental import pallas as pl
from jax.experimental.pallas import tpu as pltpu
from jax.sharding import PartitionSpec as P

F32 = jnp.float32
BF16 = jnp.bfloat16
NT = (((1,), (1,)), ((), ()))
NN = (((1,), (0,)), ((), ()))
QUAD = 4
CORES = 2
TILE = 256


def vmem_call(body, outs, scratch=(), flops=0, nbytes=0, **kw):
    many = isinstance(outs, (list, tuple))
    return pl.pallas_call(
        body,
        out_shape=outs,
        scratch_shapes=list(scratch),
        out_specs=jax.tree.map(lambda _: pl.BlockSpec(memory_space=pltpu.VMEM), tuple(outs) if many else outs),
        compiler_params=pltpu.CompilerParams(vmem_limit_bytes=32 << 20),
        cost_estimate=pl.CostEstimate(flops=flops, bytes_accessed=nbytes, transcendentals=0),
        **kw,
    )


def kernel_block(rows, centers):
    scores = lax.dot_general(rows, centers, NT, preferred_element_type=F32)
    lifted = 1.0 + 0.5 / math.sqrt(rows.shape[1]) * scores
    return (lifted * lifted * lifted).astype(BF16)


def times_kernel(low_refs, k_refs, out, low_out):
    half = k_refs[0].shape[0]
    for part in range(2):
        refs = k_refs[part::2]

        @pl.loop(0, half // TILE)
        def _(step):
            at = pl.multiple_of(step * TILE, TILE)
            total = None
            for low, ref in zip(low_refs, refs):
                term = lax.dot_general(ref[pl.ds(at, TILE), :], low, NT, preferred_element_type=F32)
                total = term if total is None else total + term
            total = total.T
            out[:, pl.ds(part * half + at, TILE)] = total
            low_out[:, pl.ds(part * half + at, TILE)] = total.astype(BF16)


def times_transposed(low_ref, k_refs, store):
    half = k_refs[0].shape[0]
    for block in range(QUAD):
        total = None
        for part in range(2):
            term = lax.dot_general(
                low_ref[:, part * half : (part + 1) * half], k_refs[2 * block + part][...], NN, preferred_element_type=F32
            )
            total = term if total is None else total + term
        store(block, total)


def first_kernel(scale, *refs):
    own, got, k_refs = refs[:QUAD], refs[QUAD : 2 * QUAD], refs[2 * QUAD : 4 * QUAD]
    right_side, partial, partial_low = refs[4 * QUAD :]
    width = own[0].shape[1]
    lows = []
    for block in range(QUAD):
        value = (own[block][...] + got[block][...]) * scale
        right_side[:, block * width : (block + 1) * width] = value
        lows.append(value.astype(BF16))
    times_kernel(lows, k_refs, partial, partial_low)


def back_kernel(last, partial, got, *refs):
    k_refs = refs[: 2 * QUAD]
    if last:
        image, image_low, squares, low = refs[2 * QUAD :]
    else:
        image, low = refs[2 * QUAD :]
    total = partial[...] + got[...].astype(F32)
    rounded = total.astype(BF16)
    low[...] = rounded
    width = k_refs[0].shape[1]
    if last:
        sums = jnp.sum(total * rounded.astype(F32), axis=1, keepdims=True)
        squares[...] = jnp.broadcast_to(sums, squares.shape)

    def store(block, value):
        image[:, block * width : (block + 1) * width] = value
        if last:
            image_low[:, block * width : (block + 1) * width] = value.astype(BF16)

    times_transposed(low, k_refs, store)


def sums_kernel(rows, own, got, right_side, image, sums):
    direction = right_side[...]
    value = (own[...] + got[...]) * (1.0 / rows) + 0.5 * direction
    image[...] = value
    for index, product in enumerate((direction * direction, direction * value, value * value)):
        sums[index] = jnp.broadcast_to(jnp.sum(product, axis=1, keepdims=True), sums.shape[1:])


def scalars(own_sums, got_sums):
    norm, curvature, image_sq = [own_sums[k][:, :1] + got_sums[k][:, :1] for k in range(3)]
    step = norm / (curvature + 1e-06)
    norm_next = norm - 2.0 * step * curvature + step * step * image_sq
    ratio = norm_next / (norm + 1e-06)
    direction_sq = norm_next + 2.0 * ratio * (norm - step * curvature) + ratio * ratio * norm
    return step, norm_next, ratio, direction_sq


def middle_kernel(own_sums, got_sums, right_side, image, *refs):
    k_refs = refs[: 2 * QUAD]
    residual, direction, partial, partial_low = refs[2 * QUAD :]
    step, _, ratio, _ = scalars(own_sums, got_sums)
    first = right_side[...]
    res = first - step * image[...]
    new = res + ratio * first
    residual[...] = res
    direction[...] = new
    low = new.astype(BF16)
    width = k_refs[0].shape[1]
    times_kernel([low[:, b * width : (b + 1) * width] for b in range(QUAD)], k_refs, partial, partial_low)


def last_kernel(rows, own_sums, got_sums, own_sq, got_sq, own, got, right_side, residual, direction, *out):
    step, norm_next, _, direction_sq = scalars(own_sums, got_sums)
    curvature = (own_sq[:, :1] + got_sq[:, :1]) * (1.0 / rows) + 0.5 * direction_sq
    step_two = norm_next / (curvature + 1e-06)
    new = direction[...]
    image = (own[...] + got[...].astype(F32)) * (1.0 / rows) + 0.5 * new
    coef = (step * right_side[...] + step_two * new).astype(BF16)
    res = (residual[...] - step_two * image).astype(BF16)
    w = coef.shape[0]
    width = out[0].shape[1]
    for block in range(QUAD):
        out[block][0:w, :] = coef[:, block * width : (block + 1) * width]
        out[block][w : 2 * w, :] = res[:, block * width : (block + 1) * width]


def place_kernel(w, place, *refs):
    mine, other = refs[:QUAD], refs[QUAD : 2 * QUAD]
    coef, residual, coef_t, residual_t = refs[2 * QUAD :]
    core, quad = place[0], place[1]
    half = coef.shape[0] // CORES
    for hop in range(QUAD):
        group = jnp.bitwise_xor(quad, hop) * CORES
        for swapped, piece, at in ((0, mine[hop], group + core), (1, other[hop], group + 1 - core)):
            rows = pl.ds(pl.multiple_of(at * w, w), w)
            for index in range(CORES):
                cols = slice(index * half, (index + 1) * half)
                source = slice((index ^ swapped) * half, ((index ^ swapped) + 1) * half)
                coef_t[rows, cols] = piece[0:w, source].astype(F32)
                residual_t[rows, cols] = piece[w : 2 * w, source].astype(F32)
    for index in range(CORES):
        at = jnp.bitwise_xor(core, index) * half
        rows = pl.ds(pl.multiple_of(at, half), half)
        coef[rows, :] = coef_t[:, index * half : (index + 1) * half].T
        residual[rows, :] = residual_t[:, index * half : (index + 1) * half].T


def on_device(features, centers, targets):
    n_dp, n_center = lax.axis_size("dp"), lax.axis_size("center")
    chips, halves = n_dp // CORES, n_center // QUAD
    dp_at, center_at = lax.axis_index("dp"), lax.axis_index("center")
    core, quad = dp_at % CORES, center_at % QUAD
    examples, columns, block = features.shape[0], targets.shape[1], centers.shape[0]
    total_rows = examples * n_dp
    w = columns // (QUAD * CORES)
    half = block // CORES

    def swap(value):
        return lax.ppermute(value, "dp", [(i, i ^ 1) for i in range(n_dp)])

    def over_quad(value, hop):
        return lax.ppermute(value, "center", [(j, j ^ hop) for j in range(n_center)])

    def others(value, axis, size, inner):
        n = size * inner
        got = None
        for shift in range(1, size):
            pairs = [(i, (i // inner + shift) % size * inner + i % inner) for i in range(n)]
            piece = lax.ppermute(value, axis, pairs)
            got = piece if got is None else got + piece
        return got

    def over_x(value):
        return others(value, "dp", chips, CORES)

    def over_halves(value):
        return others(value, "center", halves, QUAD)

    features_two = swap(features)
    mine = lax.dynamic_slice_in_dim(centers, core * half, half, 0)
    other = lax.dynamic_slice_in_dim(centers, (1 - core) * half, half, 0)
    cut = half // 2
    a, b = mine[:cut], mine[cut:]
    y_b, z_a = over_quad(b, 1), over_quad(a, 2)
    y_a, z_b = over_quad(a, 1), over_quad(b, 2)
    d_a, d_b = over_quad(z_a, 1), over_quad(y_b, 2)

    def pick(first):
        wanted = lax.broadcasted_iota(jnp.int32, (w, columns), 0) + first
        chosen = (wanted == lax.broadcasted_iota(jnp.int32, (w, columns), 1)).astype(BF16)
        return lax.dot_general(chosen, targets, NT, preferred_element_type=F32).astype(BF16)

    wanted = pick((quad * CORES + core) * w)
    wanted_two = swap(pick((quad * CORES + 1 - core) * w))

    pieces = []
    sums = []
    for rows in ((mine, other), (y_a, y_b), (z_a, z_b), (d_a, d_b)):
        if rows[0] is not mine:
            got = jnp.concatenate(rows, axis=0)
            rows = (got, swap(got))
        rows = jnp.concatenate(rows, axis=0)
        one, two = kernel_block(features, rows), kernel_block(features_two, rows)
        pieces += [one, two]
        sums.append(
            lax.dot_general(wanted, one, NN, preferred_element_type=F32)
            + lax.dot_general(wanted_two, two, NN, preferred_element_type=F32)
        )
    got_sums = [over_x(value) for value in sums]

    both, wide = CORES * examples, QUAD * block
    flops = 2 * 256 * both * wide
    sd = jax.ShapeDtypeStruct
    right_side, partial, partial_low = vmem_call(
        functools.partial(first_kernel, 1.0 / math.sqrt(total_rows)),
        [sd((w, wide), F32), sd((w, both), F32), sd((w, both), BF16)],
        flops=flops,
    )(*sums, *got_sums, *pieces)
    got = over_halves(partial_low)
    image, = vmem_call(
        functools.partial(back_kernel, False), [sd((w, wide), F32)], [pltpu.VMEM((w, both), BF16)], flops=flops
    )(partial, got, *pieces)
    got = over_x(image)
    image, dots = vmem_call(
        functools.partial(sums_kernel, total_rows), [sd((w, wide), F32), sd((3, w, 128), F32)], flops=1000000
    )(image, got, right_side)
    got_dots = over_halves(dots)
    residual, direction, partial, partial_low = vmem_call(
        middle_kernel, [sd((w, wide), F32), sd((w, wide), F32), sd((w, both), F32), sd((w, both), BF16)], flops=flops
    )(dots, got_dots, right_side, image, *pieces)
    got = over_halves(partial_low)
    image, image_low, squares = vmem_call(
        functools.partial(back_kernel, True),
        [sd((w, wide), F32), sd((w, wide), BF16), sd((w, 128), F32)],
        [pltpu.VMEM((w, both), BF16)],
        flops=flops,
    )(partial, got, *pieces)
    got, got_squares = over_x(image_low), over_x(squares)
    finals = vmem_call(
        functools.partial(last_kernel, total_rows), [sd((2 * w, block), BF16)] * QUAD, flops=1000000
    )(dots, got_dots, squares, got_squares, image, got, right_side, residual, direction)
    landed = [finals[0]] + [over_quad(finals[hop], hop) for hop in range(1, QUAD)]
    landed_two = [swap(piece) for piece in landed]
    place = jnp.stack([core, quad]).astype(jnp.int32)
    return tuple(
        vmem_call(
            functools.partial(place_kernel, w),
            [sd((block, columns), F32)] * 2,
            [pltpu.VMEM((columns, block), F32)] * 2,
            flops=1000000,
            in_specs=[pl.BlockSpec(memory_space=pltpu.SMEM)] + [pl.BlockSpec(memory_space=pltpu.VMEM)] * (2 * QUAD),
        )(place, *landed, *landed_two)
    )


def solution(mesh):
    placed = (P("dp", None), P("center", None), P("dp", None))
    return jax.shard_map(
        on_device,
        mesh=mesh,
        in_specs=placed,
        out_specs=(P("center", None), P("center", None)),
        check_vma=False,
    )
```

```python
import functools
import math

import jax
import jax.numpy as jnp
from jax import lax
from jax.experimental import pallas as pl
from jax.experimental.pallas import tpu as pltpu
from jax.sharding import PartitionSpec as P


F32 = jnp.float32
BF16 = jnp.bfloat16
NT = (((1,), (1,)), ((), ()))
NN = (((1,), (0,)), ((), ()))
QUAD = 4
CORES = 2
TILE = 256


def vmem_call(body, outs, scratch=(), flops=0, nbytes=0, **kw):
    many = isinstance(outs, (list, tuple))
    return pl.pallas_call(
        body,
        out_shape=outs,
        scratch_shapes=list(scratch),
        out_specs=jax.tree.map(lambda _: pl.BlockSpec(memory_space=pltpu.VMEM), tuple(outs) if many else outs),
        compiler_params=pltpu.CompilerParams(vmem_limit_bytes=32 << 20),
        cost_estimate=pl.CostEstimate(flops=flops, bytes_accessed=nbytes, transcendentals=0),
        **kw,
    )


def kernel_block(rows, centers):
    scores = lax.dot_general(rows, centers, NT, preferred_element_type=F32)
    lifted = 1.0 + 0.5 / math.sqrt(rows.shape[1]) * scores
    return (lifted * lifted * lifted).astype(BF16)


def times_kernel(low, parts, emit):
    half = parts[0][0].shape[0]
    for part, refs in enumerate(parts):
        for at in range(0, half, TILE):
            total, first = None, 0
            for ref in refs:
                width = ref.shape[1]
                term = lax.dot_general(
                    ref[at : at + TILE, :], low[:, first : first + width], NT, preferred_element_type=F32
                )
                total = term if total is None else total + term
                first += width
            emit(slice(part * half + at, part * half + at + TILE), total.T)


def times_transposed(lows, parts, store):
    first = 0
    for one, two in zip(*parts):
        value = lax.dot_general(lows[0], one[...], NN, preferred_element_type=F32)
        value = value + lax.dot_general(lows[1], two[...], NN, preferred_element_type=F32)
        store(slice(first, first + one.shape[1]), value)
        first += one.shape[1]


def halves_of(refs):
    return refs[: len(refs) // 2], refs[len(refs) // 2 :]


def side_kernel(count, one, two, *refs):
    out = refs[count]

    def store(cols, value):
        out[:, cols] = value

    times_transposed((one[...], two[...]), halves_of(refs[:count]), store)


def early_kernel(scale, count, own, got, *refs):
    right_side, partial = refs[count:]
    value = (own[...] + got[...]) * scale
    right_side[...] = value

    def emit(cols, value):
        partial[:, cols] = value

    times_kernel(value.astype(BF16), halves_of(refs[:count]), emit)


def late_kernel(scale, count, own, got, early_side, early, *refs):
    right_side, partial, partial_low = refs[count:]
    value = (own[...] + got[...]) * scale
    before = early_side.shape[1]
    right_side[:, :before] = early_side[...]
    right_side[:, before:] = value

    def emit(cols, value):
        value = value + early[:, cols]
        partial[:, cols] = value
        partial_low[:, cols] = value.astype(BF16)

    times_kernel(value.astype(BF16), halves_of(refs[:count]), emit)


def back_kernel(last, count, partial, got, *refs):
    if last:
        image, image_low, squares = refs[count:]
    else:
        image, = refs[count:]
    total = partial[...] + got[...].astype(F32)
    low = total.astype(BF16)
    if last:
        sums = jnp.sum(total * low.astype(F32), axis=1, keepdims=True)
        squares[...] = jnp.broadcast_to(sums, squares.shape)

    def store(cols, value):
        image[:, cols] = value
        if last:
            image_low[:, cols] = value.astype(BF16)

    half = low.shape[1] // 2
    times_transposed((low[:, :half], low[:, half:]), halves_of(refs[:count]), store)


def sums_kernel(rows, own, got, right_side, image, sums):
    direction = right_side[...]
    value = (own[...] + got[...]) * (1.0 / rows) + 0.5 * direction
    image[...] = value
    for index, product in enumerate((direction * direction, direction * value, value * value)):
        sums[index] = jnp.broadcast_to(jnp.sum(product, axis=1, keepdims=True), sums.shape[1:])


def scalars(own_sums, got_sums):
    norm, curvature, image_sq = [own_sums[k][:, :1] + got_sums[k][:, :1] for k in range(3)]
    step = norm / (curvature + 1e-06)
    norm_next = norm - 2.0 * step * curvature + step * step * image_sq
    ratio = norm_next / (norm + 1e-06)
    direction_sq = norm_next + 2.0 * ratio * (norm - step * curvature) + ratio * ratio * norm
    return step, norm_next, ratio, direction_sq


def middle_kernel(count, own_sums, got_sums, right_side, image, *refs):
    residual, direction, partial, partial_low = refs[count:]
    step, _, ratio, _ = scalars(own_sums, got_sums)
    first = right_side[...]
    res = first - step * image[...]
    new = res + ratio * first
    residual[...] = res
    direction[...] = new

    def emit(cols, value):
        partial[:, cols] = value
        partial_low[:, cols] = value.astype(BF16)

    times_kernel(new.astype(BF16), halves_of(refs[:count]), emit)


def last_kernel(rows, own_sums, got_sums, own_sq, got_sq, own, got, right_side, residual, direction, *out):
    step, norm_next, _, direction_sq = scalars(own_sums, got_sums)
    curvature = (own_sq[:, :1] + got_sq[:, :1]) * (1.0 / rows) + 0.5 * direction_sq
    step_two = norm_next / (curvature + 1e-06)
    new = direction[...]
    image = (own[...] + got[...].astype(F32)) * (1.0 / rows) + 0.5 * new
    coef = (step * right_side[...] + step_two * new).astype(BF16)
    res = (residual[...] - step_two * image).astype(BF16)
    w = coef.shape[0]
    width = out[0].shape[1]
    for block in range(QUAD):
        out[block][0:w, :] = coef[:, block * width : (block + 1) * width]
        out[block][w : 2 * w, :] = res[:, block * width : (block + 1) * width]


def place_kernel(w, place, *refs):
    mine, other = refs[:QUAD], refs[QUAD : 2 * QUAD]
    coef, residual, coef_t, residual_t = refs[2 * QUAD :]
    core, quad = place[0], place[1]
    half = coef.shape[0] // CORES
    for hop in range(QUAD):
        group = jnp.bitwise_xor(quad, hop) * CORES
        for swapped, piece, at in ((0, mine[hop], group + core), (1, other[hop], group + 1 - core)):
            rows = pl.ds(pl.multiple_of(at * w, w), w)
            for index in range(CORES):
                to = index if hop == 0 else jnp.bitwise_xor(core, index ^ swapped)
                cols = pl.ds(pl.multiple_of(to * half, half), half)
                source = slice(index * half, (index + 1) * half)
                coef_t[rows, cols] = piece[0:w, source].astype(F32)
                residual_t[rows, cols] = piece[w : 2 * w, source].astype(F32)
    coef[...] = coef_t[...].T
    residual[...] = residual_t[...].T


def split_kernel(place, centers, mine, sem):
    half = mine.shape[0]
    at = pl.multiple_of(place[0] * half, half)
    copy = pltpu.make_async_copy(centers.at[pl.ds(at, half), :], mine, sem)
    copy.start()
    copy.wait()


def load_kernel(features, out, sem):
    copy = pltpu.make_async_copy(features, out, sem)
    copy.start()
    copy.wait()


def on_device(features, centers, targets):
    n_dp, n_center = lax.axis_size("dp"), lax.axis_size("center")
    chips, halves = n_dp // CORES, n_center // QUAD
    dp_at, center_at = lax.axis_index("dp"), lax.axis_index("center")
    core, quad = dp_at % CORES, center_at % QUAD
    examples, columns, block = features.shape[0], targets.shape[1], centers.shape[0]
    total_rows = examples * n_dp
    w = columns // (QUAD * CORES)
    half = block // CORES

    def swap(value):
        return lax.ppermute(value, "dp", [(i, i ^ 1) for i in range(n_dp)])

    def over_quad(value, hop):
        return lax.ppermute(value, "center", [(j, j ^ hop) for j in range(n_center)])

    def others(value, axis, size, inner):
        n = size * inner
        got = None
        for shift in range(1, size):
            pairs = [(i, (i // inner + shift) % size * inner + i % inner) for i in range(n)]
            piece = lax.ppermute(value, axis, pairs)
            got = piece if got is None else got + piece
        return got

    def over_x(value):
        return others(value, "dp", chips, CORES)

    def over_halves(value):
        return others(value, "center", halves, QUAD)

    sd = jax.ShapeDtypeStruct
    place = jnp.stack([core, quad]).astype(jnp.int32)
    depth = centers.shape[1]
    mine, = vmem_call(
        split_kernel,
        [sd((half, depth), BF16)],
        [pltpu.SemaphoreType.DMA(())],
        flops=1000000,
        in_specs=[pl.BlockSpec(memory_space=pltpu.SMEM), pl.BlockSpec(memory_space=pl.ANY)],
    )(place, centers)
    y_mine = over_quad(mine, 1)
    z_mine = over_quad(mine, 2)
    features_two = swap(features)
    features_two, = vmem_call(
        load_kernel,
        [sd(features.shape, BF16)],
        [pltpu.SemaphoreType.DMA(())],
        flops=1000000,
        in_specs=[pl.BlockSpec(memory_space=pl.ANY)],
    )(features_two)

    def pick(first):
        wanted = lax.broadcasted_iota(jnp.int32, (w, columns), 0) + first
        chosen = (wanted == lax.broadcasted_iota(jnp.int32, (w, columns), 1)).astype(BF16)
        return lax.dot_general(chosen, targets, NT, preferred_element_type=F32).astype(BF16)

    wanted_two = swap(pick((quad * CORES + 1 - core) * w))
    wanted = pick((quad * CORES + core) * w)

    def build(rows):
        return kernel_block(features, rows), kernel_block(features_two, rows)

    own = build(centers)
    pairs = []
    for i in range(n_dp):
        hop = 1 if i % CORES == 0 else 2
        pairs += [(i * n_center + j, i * n_center + (j ^ hop)) for j in range(n_center)]
    d_mine = lax.ppermute(jnp.where(core == 0, z_mine, y_mine), ("dp", "center"), pairs)
    y_other = swap(y_mine)
    z_other = swap(z_mine)
    y_0, z_0 = build(y_mine), build(z_mine)
    y_1, z_1 = build(y_other), build(z_other)
    early_pieces = [p[side] for side in range(2) for p in (own, y_0, y_1, z_0, z_1)]

    both, wide = CORES * examples, QUAD * block
    flops = 2 * 256 * both * wide
    side, = vmem_call(
        functools.partial(side_kernel, len(early_pieces)), [sd((w, wide - block), F32)], flops=flops * 3 // 4
    )(wanted, wanted_two, *early_pieces)
    got_side = over_x(side)
    d_other = swap(d_mine)
    d_0 = build(d_mine)
    d_1 = build(d_other)
    late_pieces = [p[side] for side in range(2) for p in (d_0, d_1)]
    late, = vmem_call(
        functools.partial(side_kernel, len(late_pieces)), [sd((w, block), F32)], flops=flops // 4
    )(wanted, wanted_two, *late_pieces)
    got_late = over_x(late)

    scale = 1.0 / math.sqrt(total_rows)
    early_side, early = vmem_call(
        functools.partial(early_kernel, scale, len(early_pieces)),
        [sd((w, wide - block), F32), sd((w, both), F32)],
        flops=flops * 3 // 4,
    )(side, got_side, *early_pieces)
    right_side, partial, partial_low = vmem_call(
        functools.partial(late_kernel, scale, len(late_pieces)),
        [sd((w, wide), F32), sd((w, both), F32), sd((w, both), BF16)],
        flops=flops // 4,
    )(late, got_late, early_side, early, *late_pieces)
    pieces = [
        piece for part in zip(halves_of(early_pieces), halves_of(late_pieces)) for group in part for piece in group
    ]
    count = len(pieces)
    got = over_halves(partial_low)
    image, = vmem_call(functools.partial(back_kernel, False, count), [sd((w, wide), F32)], flops=flops)(
        partial, got, *pieces
    )
    got = over_x(image)
    image, dots = vmem_call(
        functools.partial(sums_kernel, total_rows), [sd((w, wide), F32), sd((3, w, 128), F32)], flops=1000000
    )(image, got, right_side)
    got_dots = over_halves(dots)
    residual, direction, partial, partial_low = vmem_call(
        functools.partial(middle_kernel, count), [sd((w, wide), F32), sd((w, wide), F32), sd((w, both), F32), sd((w, both), BF16)], flops=flops
    )(dots, got_dots, right_side, image, *pieces)
    got = over_halves(partial_low)
    image, image_low, squares = vmem_call(
        functools.partial(back_kernel, True, count),
        [sd((w, wide), F32), sd((w, wide), BF16), sd((w, 128), F32)],
        flops=flops,
    )(partial, got, *pieces)
    got, got_squares = over_x(image_low), over_x(squares)
    finals = vmem_call(
        functools.partial(last_kernel, total_rows), [sd((2 * w, block), BF16)] * QUAD, flops=1000000
    )(dots, got_dots, squares, got_squares, image, got, right_side, residual, direction)
    landed = [finals[0]] + [over_quad(finals[hop], hop) for hop in range(1, QUAD)]
    landed_two = [swap(piece) for piece in landed]
    return tuple(
        vmem_call(
            functools.partial(place_kernel, w),
            [sd((block, columns), F32)] * 2,
            [pltpu.VMEM((columns, block), F32)] * 2,
            flops=1000000,
            in_specs=[pl.BlockSpec(memory_space=pltpu.SMEM)] + [pl.BlockSpec(memory_space=pltpu.VMEM)] * (2 * QUAD),
        )(place, *landed, *landed_two)
    )


def solution(mesh):
    placed = (P("dp", None), P("center", None), P("dp", None))
    return jax.shard_map(
        on_device,
        mesh=mesh,
        in_specs=placed,
        out_specs=(P("center", None), P("center", None)),
        check_vma=False,
    )
```

```python
import functools
import math

import jax
import jax.numpy as jnp
from jax import lax
from jax.experimental import pallas as pl
from jax.experimental.pallas import tpu as pltpu
from jax.sharding import PartitionSpec as P


F32 = jnp.float32
BF16 = jnp.bfloat16
NT = (((1,), (1,)), ((), ()))
NN = (((1,), (0,)), ((), ()))
QUAD = 4
CORES = 2
TILE = 256
CHUNKS = 2


def vmem_call(body, outs, scratch=(), flops=0, nbytes=0, limit=32 << 20, **kw):
    many = isinstance(outs, (list, tuple))
    return pl.pallas_call(
        body,
        out_shape=outs,
        scratch_shapes=list(scratch),
        out_specs=jax.tree.map(lambda _: pl.BlockSpec(memory_space=pltpu.VMEM), tuple(outs) if many else outs),
        compiler_params=pltpu.CompilerParams(vmem_limit_bytes=limit),
        cost_estimate=pl.CostEstimate(flops=flops, bytes_accessed=nbytes, transcendentals=0),
        **kw,
    )


def kernel_block(rows, centers):
    scores = lax.dot_general(rows, centers, NT, preferred_element_type=F32)
    lifted = 1.0 + 0.5 / math.sqrt(rows.shape[1]) * scores
    return (lifted * lifted * lifted).astype(BF16)


def times_kernel(low, parts, emit):
    half = parts[0][0].shape[0]
    for part, refs in enumerate(parts):
        for at in range(0, half, TILE):
            total, first = None, 0
            for ref in refs:
                width = ref.shape[1]
                term = lax.dot_general(
                    ref[at : at + TILE, :], low[:, first : first + width], NT, preferred_element_type=F32
                )
                total = term if total is None else total + term
                first += width
            emit(slice(part * half + at, part * half + at + TILE), total.T)


def times_transposed(lows, parts, store):
    first = 0
    for one, two in zip(*parts):
        value = lax.dot_general(lows[0], one[...], NN, preferred_element_type=F32)
        value = value + lax.dot_general(lows[1], two[...], NN, preferred_element_type=F32)
        store(slice(first, first + one.shape[1]), value)
        first += one.shape[1]


def halves_of(refs):
    return refs[: len(refs) // 2], refs[len(refs) // 2 :]


def side_kernel(count, one, two, *refs):
    out = refs[count]

    def store(cols, value):
        out[:, cols] = value

    times_transposed((one[...], two[...]), halves_of(refs[:count]), store)


def right_kernel(scale, own, got, *out):
    w = out[0].shape[0]
    for hop in range(QUAD):
        rows = slice(hop * w, (hop + 1) * w)
        out[hop][...] = (own[rows, :] + got[rows, :]) * scale


def segments():
    found = []
    for chunk in range(CHUNKS):
        for far in range(CORES):
            found += [(1, far, chunk), (2, far, chunk)]
    for far in range(CORES):
        found += [(3, far, chunk) for chunk in range(CHUNKS)]
    return found


def early_kernel(count, n_early, *refs):
    sides, k_refs = refs[:QUAD], refs[QUAD : QUAD + count]
    right_side, low_last, partial = refs[QUAD + count :]
    core = lax.axis_index("dp") % CORES
    width = sides[0].shape[1]
    half = width // CORES
    cut = half // CHUNKS
    right_side[:, :width] = sides[0][...]
    for index, (hop, far, chunk) in enumerate(segments()):
        at = pl.multiple_of(jnp.bitwise_xor(core, far) * half + chunk * cut, cut)
        to = width + index * cut
        right_side[:, to : to + cut] = sides[hop][:, pl.ds(at, cut)]
    low_last[...] = right_side[:, n_early:].astype(BF16)

    def emit(cols, value):
        partial[:, cols] = value

    times_kernel(right_side[:, :n_early].astype(BF16), halves_of(k_refs), emit)


def late_kernel(count, low, early, *refs):
    partial, partial_low = refs[count:]

    def emit(cols, value):
        value = value + early[:, cols]
        partial[:, cols] = value
        partial_low[:, cols] = value.astype(BF16)

    times_kernel(low, halves_of(refs[:count]), emit)


def back_kernel(last, count, partial, got, *refs):
    if last:
        image, image_low, squares = refs[count:]
    else:
        image, = refs[count:]
    total = partial[...] + got[...].astype(F32)
    low = total.astype(BF16)
    if last:
        sums = jnp.sum(total * low.astype(F32), axis=1, keepdims=True)
        squares[...] = jnp.broadcast_to(sums, squares.shape)

    def store(cols, value):
        image[:, cols] = value
        if last:
            image_low[:, cols] = value.astype(BF16)

    half = low.shape[1] // 2
    times_transposed((low[:, :half], low[:, half:]), halves_of(refs[:count]), store)


def sums_kernel(rows, own, got, right_side, image, sums):
    direction = right_side[...]
    value = (own[...] + got[...]) * (1.0 / rows) + 0.5 * direction
    image[...] = value
    for index, product in enumerate((direction * direction, direction * value, value * value)):
        sums[index] = jnp.broadcast_to(jnp.sum(product, axis=1, keepdims=True), sums.shape[1:])


def scalars(own_sums, got_sums):
    norm, curvature, image_sq = [own_sums[k][:, :1] + got_sums[k][:, :1] for k in range(3)]
    step = norm / (curvature + 1e-06)
    norm_next = norm - 2.0 * step * curvature + step * step * image_sq
    ratio = norm_next / (norm + 1e-06)
    direction_sq = norm_next + 2.0 * ratio * (norm - step * curvature) + ratio * ratio * norm
    return step, norm_next, ratio, direction_sq


def middle_kernel(count, own_sums, got_sums, right_side, image, *refs):
    residual, direction, partial, partial_low = refs[count:]
    step, _, ratio, _ = scalars(own_sums, got_sums)
    first = right_side[...]
    res = first - step * image[...]
    new = res + ratio * first
    residual[...] = res
    direction[...] = new

    def emit(cols, value):
        partial[:, cols] = value
        partial_low[:, cols] = value.astype(BF16)

    times_kernel(new.astype(BF16), halves_of(refs[:count]), emit)


def last_kernel(rows, own_sums, got_sums, own_sq, got_sq, own, got, right_side, residual, direction, *out):
    step, norm_next, _, direction_sq = scalars(own_sums, got_sums)
    curvature = (own_sq[:, :1] + got_sq[:, :1]) * (1.0 / rows) + 0.5 * direction_sq
    step_two = norm_next / (curvature + 1e-06)
    new = direction[...]
    image = (own[...] + got[...].astype(F32)) * (1.0 / rows) + 0.5 * new
    coef = (step * right_side[...] + step_two * new).astype(BF16)
    res = (residual[...] - step_two * image).astype(BF16)
    w = coef.shape[0]
    width = out[0].shape[1]
    half = width // CORES
    cut = half // CHUNKS
    for first, value in ((0, coef), (w, res)):
        rows = slice(first, first + w)
        out[0][rows, :] = value[:, :width]
        for index, (hop, far, chunk) in enumerate(segments()):
            at, to = width + index * cut, far * half + chunk * cut
            out[hop][rows, to : to + cut] = value[:, at : at + cut]


def place_kernel(w, place, *refs):
    mine, other = refs[:QUAD], refs[QUAD : 2 * QUAD]
    coef, residual, coef_t, residual_t = refs[2 * QUAD :]
    core, quad = place[0], place[1]
    half = coef.shape[0] // CORES
    for hop in range(QUAD):
        group = jnp.bitwise_xor(quad, hop) * CORES
        for swapped, piece, at in ((0, mine[hop], group + core), (1, other[hop], group + 1 - core)):
            rows = pl.ds(pl.multiple_of(at * w, w), w)
            for index in range(CORES):
                to = index if hop == 0 else jnp.bitwise_xor(core, index ^ swapped)
                cols = pl.ds(pl.multiple_of(to * half, half), half)
                source = slice(index * half, (index + 1) * half)
                coef_t[rows, cols] = piece[0:w, source].astype(F32)
                residual_t[rows, cols] = piece[w : 2 * w, source].astype(F32)
    coef[...] = coef_t[...].T
    residual[...] = residual_t[...].T


def run(copies):
    for copy in copies:
        copy.start()
    for copy in copies:
        copy.wait()


def split_kernel(centers, *refs):
    chunks, sems = refs[:-1], refs[-1]
    cut = chunks[0].shape[0]
    at = (lax.axis_index("dp") % CORES) * (cut * CHUNKS)
    run(
        [
            pltpu.make_async_copy(centers.at[pl.ds(pl.multiple_of(at + k * cut, cut), cut), :], chunk, sems.at[k])
            for k, chunk in enumerate(chunks)
        ]
    )


def keep_kernel(value, out, sem):
    run([pltpu.make_async_copy(value, out, sem)])


def fork_kernel(y, z, both, send, sems):
    cut = y.shape[0]
    copies = [
        pltpu.make_async_copy(y, both.at[pl.ds(0, cut), :], sems.at[0]),
        pltpu.make_async_copy(z, both.at[pl.ds(cut, cut), :], sems.at[1]),
    ]
    for copy in copies:
        copy.start()
    core = lax.axis_index("dp") % CORES

    @pl.when(core == 0)
    def _():
        run([pltpu.make_async_copy(z, send, sems.at[2])])

    @pl.when(core != 0)
    def _():
        run([pltpu.make_async_copy(y, send, sems.at[2])])

    for copy in copies:
        copy.wait()


def join_kernel(a, b, both, sems):
    cut = a.shape[0]
    run(
        [
            pltpu.make_async_copy(a, both.at[pl.ds(0, cut), :], sems.at[0]),
            pltpu.make_async_copy(b, both.at[pl.ds(cut, cut), :], sems.at[1]),
        ]
    )


def on_device(features, centers, targets):
    n_dp, n_center = lax.axis_size("dp"), lax.axis_size("center")
    chips, halves = n_dp // CORES, n_center // QUAD
    dp_at, center_at = lax.axis_index("dp"), lax.axis_index("center")
    core, quad = dp_at % CORES, center_at % QUAD
    examples, columns, block = features.shape[0], targets.shape[1], centers.shape[0]
    total_rows = examples * n_dp
    w = columns // (QUAD * CORES)
    half = block // CORES

    def swap(value):
        return lax.ppermute(value, "dp", [(i, i ^ 1) for i in range(n_dp)])

    def over_quad(value, hop):
        return lax.ppermute(value, "center", [(j, j ^ hop) for j in range(n_center)])

    def others(value, axis, size, inner):
        n = size * inner
        got = None
        for shift in range(1, size):
            pairs = [(i, (i // inner + shift) % size * inner + i % inner) for i in range(n)]
            piece = lax.ppermute(value, axis, pairs)
            got = piece if got is None else got + piece
        return got

    def over_x(value):
        return others(value, "dp", chips, CORES)

    def over_halves(value):
        return others(value, "center", halves, QUAD)

    sd = jax.ShapeDtypeStruct
    place = jnp.stack([core, quad]).astype(jnp.int32)
    depth = centers.shape[1]
    mine_size = half * depth
    any_space = pl.BlockSpec(memory_space=pl.ANY)
    cut = half // CHUNKS
    chunks = vmem_call(
        split_kernel,
        [sd((cut, depth), BF16)] * CHUNKS,
        [pltpu.SemaphoreType.DMA((CHUNKS,))],
        flops=1000000,
        limit=(64 << 20) - 2 * (mine_size + targets.size) - (1 << 19),
        in_specs=[any_space],
    )(centers)
    y_in, z_in = [], []
    for k in range(CHUNKS):
        y_in.append(over_quad(chunks[k], 1))
        z_in.append(over_quad(chunks[k], 2))
    features_two = swap(features)
    features_two, = vmem_call(
        keep_kernel,
        [pltpu.VMEM(features.shape, BF16)],
        [pltpu.SemaphoreType.DMA(())],
        flops=1000000,
        in_specs=[any_space],
    )(features_two)

    def pick(of_core):
        row = lax.broadcasted_iota(jnp.int32, (QUAD * w, columns), 0)
        wanted = ((quad ^ (row // w)) * CORES + of_core) * w + row % w
        chosen = (wanted == lax.broadcasted_iota(jnp.int32, (QUAD * w, columns), 1)).astype(BF16)
        return lax.dot_general(chosen, targets, NT, preferred_element_type=F32).astype(BF16)

    wanted_two = swap(pick(1 - core))
    wanted = pick(core)

    def build(rows):
        return kernel_block(features, rows), kernel_block(features_two, rows)

    own = build(centers)
    both, wide = CORES * examples, QUAD * block
    flops = 2 * 256 * both * wide
    side, = vmem_call(functools.partial(side_kernel, 2), [sd((QUAD * w, block), F32)], flops=flops // 4)(
        wanted, wanted_two, *own
    )
    got_side = over_x(side)
    pairs = []
    for i in range(n_dp):
        hop = 1 if i % CORES == 0 else 2
        pairs += [(i * n_center + j, i * n_center + (j ^ hop)) for j in range(n_center)]
    early_groups, d_in = [own], []
    for k in range(CHUNKS):
        near, d_send = vmem_call(
            fork_kernel,
            [pltpu.VMEM((2 * cut, depth), BF16), pltpu.VMEM((cut, depth), BF16)],
            [pltpu.SemaphoreType.DMA((3,))],
            flops=1000000,
            in_specs=[any_space] * 2,
        )(y_in[k], z_in[k])
        d_in.append(lax.ppermute(d_send, ("dp", "center"), pairs))
        far = swap(near)
        early_groups.append(build(near))
        early_groups.append(build(far))
    sides = vmem_call(
        functools.partial(right_kernel, 1.0 / math.sqrt(total_rows)), [sd((w, block), F32)] * QUAD, flops=1000000
    )(side, got_side)
    sides = [sides[0]] + [over_quad(sides[hop], hop) for hop in range(1, QUAD)]
    early_pieces = [p[side] for side in range(2) for p in early_groups]
    d_near, = vmem_call(
        join_kernel,
        [pltpu.VMEM((half, depth), BF16)],
        [pltpu.SemaphoreType.DMA((2,))],
        flops=1000000,
        in_specs=[any_space] * 2,
    )(*d_in)
    d_far = swap(d_near)
    d_0 = build(d_near)
    d_1 = build(d_far)
    late_pieces = [p[side] for side in range(2) for p in (d_0, d_1)]
    count = len(early_pieces)
    right_side, low_last, early = vmem_call(
        functools.partial(early_kernel, count, wide - block),
        [sd((w, wide), F32), sd((w, block), BF16), sd((w, both), F32)],
        flops=flops * 3 // 4,
    )(*sides, *early_pieces)
    partial, partial_low = vmem_call(
        functools.partial(late_kernel, len(late_pieces)),
        [sd((w, both), F32), sd((w, both), BF16)],
        flops=flops // 4,
    )(low_last, early, *late_pieces)
    pieces = [
        piece for part in zip(halves_of(early_pieces), halves_of(late_pieces)) for group in part for piece in group
    ]
    count = len(pieces)
    got = over_halves(partial_low)
    image, = vmem_call(functools.partial(back_kernel, False, count), [sd((w, wide), F32)], flops=flops)(
        partial, got, *pieces
    )
    got = over_x(image)
    image, dots = vmem_call(
        functools.partial(sums_kernel, total_rows), [sd((w, wide), F32), sd((3, w, 128), F32)], flops=1000000
    )(image, got, right_side)
    got_dots = over_halves(dots)
    residual, direction, partial, partial_low = vmem_call(
        functools.partial(middle_kernel, count), [sd((w, wide), F32), sd((w, wide), F32), sd((w, both), F32), sd((w, both), BF16)], flops=flops
    )(dots, got_dots, right_side, image, *pieces)
    got = over_halves(partial_low)
    image, image_low, squares = vmem_call(
        functools.partial(back_kernel, True, count),
        [sd((w, wide), F32), sd((w, wide), BF16), sd((w, 128), F32)],
        flops=flops,
    )(partial, got, *pieces)
    got, got_squares = over_x(image_low), over_x(squares)
    finals = vmem_call(
        functools.partial(last_kernel, total_rows), [sd((2 * w, block), BF16)] * QUAD, flops=1000000
    )(dots, got_dots, squares, got_squares, image, got, right_side, residual, direction)
    landed = [finals[0]] + [over_quad(finals[hop], hop) for hop in range(1, QUAD)]
    landed_two = [swap(piece) for piece in landed]
    return tuple(
        vmem_call(
            functools.partial(place_kernel, w),
            [sd((block, columns), F32)] * 2,
            [pltpu.VMEM((columns, block), F32)] * 2,
            flops=1000000,
            in_specs=[pl.BlockSpec(memory_space=pltpu.SMEM)] + [pl.BlockSpec(memory_space=pltpu.VMEM)] * (2 * QUAD),
        )(place, *landed, *landed_two)
    )


def solution(mesh):
    placed = (P("dp", None), P("center", None), P("dp", None))
    return jax.shard_map(
        on_device,
        mesh=mesh,
        in_specs=placed,
        out_specs=(P("center", None), P("center", None)),
        check_vma=False,
    )
```

```python
import functools
import math

import jax
import jax.numpy as jnp
from jax import lax
from jax.experimental import pallas as pl
from jax.experimental.pallas import tpu as pltpu
from jax.sharding import PartitionSpec as P


F32 = jnp.float32
BF16 = jnp.bfloat16
NT = (((1,), (1,)), ((), ()))
NN = (((1,), (0,)), ((), ()))
QUAD = 4
CORES = 2
TILE = 256
CHUNKS = 2
LANES = 128
WORDS = 3


def vmem_call(body, outs, scratch=(), flops=0, nbytes=0, limit=32 << 20, **kw):
    many = isinstance(outs, (list, tuple))
    return pl.pallas_call(
        body,
        out_shape=outs,
        scratch_shapes=list(scratch),
        out_specs=jax.tree.map(lambda _: pl.BlockSpec(memory_space=pltpu.VMEM), tuple(outs) if many else outs),
        compiler_params=pltpu.CompilerParams(vmem_limit_bytes=limit),
        cost_estimate=pl.CostEstimate(flops=flops, bytes_accessed=nbytes, transcendentals=0),
        **kw,
    )


def kernel_block(rows, centers):
    scores = lax.dot_general(rows, centers, NT, preferred_element_type=F32)
    lifted = 1.0 + 0.5 / math.sqrt(rows.shape[1]) * scores
    return (lifted * lifted * lifted).astype(BF16)


def times_kernel(low, refs, emit):
    for at in range(0, refs[0].shape[0], TILE):
        total, first = None, 0
        for ref in refs:
            width = ref.shape[1]
            term = lax.dot_general(
                ref[at : at + TILE, :], low[:, first : first + width], NT, preferred_element_type=F32
            )
            total = term if total is None else total + term
            first += width
        emit(slice(at, at + TILE), total.T)


def times_transposed(low, refs, store):
    first = 0
    for ref in refs:
        value = lax.dot_general(low, ref[...], NN, preferred_element_type=F32)
        store(slice(first, first + ref.shape[1]), value)
        first += ref.shape[1]


def side_kernel(first, second, one, two, out):
    out[...] = lax.dot_general(first[...], one[...], NN, preferred_element_type=F32)
    out[...] += lax.dot_general(second[...], two[...], NN, preferred_element_type=F32)


def right_kernel(scale, own, got, *out):
    w = out[0].shape[0]
    for hop in range(QUAD):
        rows = slice(hop * w, (hop + 1) * w)
        out[hop][...] = (own[rows, :] + got[rows, :]) * scale


def segments():
    found = []
    for chunk in range(CHUNKS):
        for far in range(CORES):
            found += [(1, far, chunk), (2, far, chunk)]
    for far in range(CORES):
        found += [(3, far, chunk) for chunk in range(CHUNKS)]
    return found


def early_kernel(count, n_early, *refs):
    sides, k_refs = refs[:QUAD], refs[QUAD : QUAD + count]
    right_side, low_last, partial = refs[QUAD + count :]
    core = lax.axis_index("dp") % CORES
    width = sides[0].shape[1]
    half = width // CORES
    cut = half // CHUNKS
    right_side[:, :width] = sides[0][...]
    for index, (hop, far, chunk) in enumerate(segments()):
        at = pl.multiple_of(jnp.bitwise_xor(core, far) * half + chunk * cut, cut)
        to = width + index * cut
        right_side[:, to : to + cut] = sides[hop][:, pl.ds(at, cut)]
    low_last[...] = right_side[:, n_early:].astype(BF16)

    def emit(cols, value):
        partial[:, cols] = value

    times_kernel(right_side[:, :n_early].astype(BF16), k_refs, emit)


def late_kernel(low, early, *refs):
    k_refs, (partial, partial_low) = refs[:-2], refs[-2:]

    def emit(cols, value):
        value = value + early[:, cols]
        partial[:, cols] = value
        partial_low[:, cols] = value.astype(BF16)

    times_kernel(low, k_refs, emit)


def second_kernel(direction, *refs):
    k_refs, (partial, partial_low) = refs[:-2], refs[-2:]

    def emit(cols, value):
        partial[:, cols] = value
        partial_low[:, cols] = value.astype(BF16)

    times_kernel(direction[...].astype(BF16), k_refs, emit)


def rounded(partial, got):
    total = partial[...] + got[...].astype(F32)
    low = total.astype(BF16)
    return low, jnp.sum(total * low.astype(F32), axis=1, keepdims=True)


def back_kernel(partial, got, *refs):
    k_refs, (image, squares) = refs[:-2], refs[-2:]
    low, sums = rounded(partial, got)
    squares[...] = jnp.broadcast_to(sums, squares.shape)

    def store(cols, value):
        image[:, cols] = value

    times_transposed(low, k_refs, store)


def back_rest_kernel(partial, got, before, *refs):
    k_refs, image = refs[:-1], refs[-1]
    low, _ = rounded(partial, got)

    def store(cols, value):
        image[:, cols] = before[:, cols] + value

    times_transposed(low, k_refs, store)


def back_last_kernel(partial, got, before, squares, *refs):
    k_refs, (image, image_low) = refs[:-2], refs[-2:]
    low, left = rounded(partial, got)
    left = left + squares[:, :1]
    tail = image_low.shape[1] - LANES
    lane = lax.broadcasted_iota(jnp.int32, (left.shape[0], LANES), 1)
    words = jnp.zeros(lane.shape, F32)
    for index in range(WORDS):
        word = left.astype(BF16).astype(F32)
        words = jnp.where(lane == index, word, words)
        left = left - word
    image_low[:, tail:] = words.astype(BF16)

    def store(cols, value):
        value = before[:, cols] + value
        image[:, cols] = value
        image_low[:, cols] = value.astype(BF16)

    times_transposed(low, k_refs, store)


def sums_kernel(rows, own, got, right_side, image, sums):
    direction = right_side[...]
    value = (own[...] + got[...]) * (1.0 / rows) + 0.5 * direction
    image[...] = value
    lane = lax.broadcasted_iota(jnp.int32, sums.shape, 1)
    found = jnp.zeros(sums.shape, F32)
    for index, product in enumerate((direction * direction, direction * value, value * value)):
        found = jnp.where(lane == index, jnp.sum(product, axis=1, keepdims=True), found)
    sums[...] = found


def scalars(own_sums, got_sums):
    total = own_sums[...] + got_sums[...]
    norm, curvature, image_sq = [total[:, k : k + 1] for k in range(3)]
    step = norm / (curvature + 1e-06)
    norm_next = norm - 2.0 * step * curvature + step * step * image_sq
    ratio = norm_next / (norm + 1e-06)
    direction_sq = norm_next + 2.0 * ratio * (norm - step * curvature) + ratio * ratio * norm
    return step, norm_next, ratio, direction_sq


def middle_kernel(own_sums, got_sums, right_side, image, *refs):
    k_refs, (residual, direction, partial, partial_low) = refs[:-4], refs[-4:]
    step, _, ratio, _ = scalars(own_sums, got_sums)
    first = right_side[...]
    res = first - step * image[...]
    new = res + ratio * first
    residual[...] = res
    direction[...] = new

    def emit(cols, value):
        partial[:, cols] = value
        partial_low[:, cols] = value.astype(BF16)

    times_kernel(new.astype(BF16), k_refs, emit)


def last_kernel(rows, own_sums, got_sums, low, own, got, right_side, residual, direction, *out):
    step, norm_next, _, direction_sq = scalars(own_sums, got_sums)
    wide = own.shape[1]
    squares = low[:, wide:].astype(F32) + got[:, wide:].astype(F32)
    curvature = jnp.sum(squares, axis=1, keepdims=True) * (1.0 / rows) + 0.5 * direction_sq
    step_two = norm_next / (curvature + 1e-06)
    new = direction[...]
    image = (own[...] + got[:, :wide].astype(F32)) * (1.0 / rows) + 0.5 * new
    coef = (step * right_side[...] + step_two * new).astype(BF16)
    res = (residual[...] - step_two * image).astype(BF16)
    w = coef.shape[0]
    width = out[0].shape[1]
    half = width // CORES
    cut = half // CHUNKS
    for first, value in ((0, coef), (w, res)):
        rows = slice(first, first + w)
        out[0][rows, :] = value[:, :width]
        for index, (hop, far, chunk) in enumerate(segments()):
            at, to = width + index * cut, far * half + chunk * cut
            out[hop][rows, to : to + cut] = value[:, at : at + cut]


def place_kernel(w, place, *refs):
    mine, other = refs[:QUAD], refs[QUAD : 2 * QUAD]
    coef, residual, coef_t, residual_t = refs[2 * QUAD :]
    core, quad = place[0], place[1]
    half = coef.shape[0] // CORES
    for hop in range(QUAD):
        group = jnp.bitwise_xor(quad, hop) * CORES
        for swapped, piece, at in ((0, mine[hop], group + core), (1, other[hop], group + 1 - core)):
            rows = pl.ds(pl.multiple_of(at * w, w), w)
            for index in range(CORES):
                to = index if hop == 0 else jnp.bitwise_xor(core, index ^ swapped)
                cols = pl.ds(pl.multiple_of(to * half, half), half)
                source = slice(index * half, (index + 1) * half)
                coef_t[rows, cols] = piece[0:w, source]
                residual_t[rows, cols] = piece[w : 2 * w, source]
    coef[...] = coef_t[...].T.astype(F32)
    residual[...] = residual_t[...].T.astype(F32)


def run(copies):
    for copy in copies:
        copy.start()
    for copy in copies:
        copy.wait()


def split_kernel(centers, *refs):
    chunks, sems = refs[:-1], refs[-1]
    cut = chunks[0].shape[0]
    at = (lax.axis_index("dp") % CORES) * (cut * CHUNKS)
    run(
        [
            pltpu.make_async_copy(centers.at[pl.ds(pl.multiple_of(at + k * cut, cut), cut), :], chunk, sems.at[k])
            for k, chunk in enumerate(chunks)
        ]
    )


def keep_kernel(value, out, sem):
    run([pltpu.make_async_copy(value, out, sem)])


def fork_kernel(y, z, both, send, sems):
    cut = y.shape[0]
    copies = [
        pltpu.make_async_copy(y, both.at[pl.ds(0, cut), :], sems.at[0]),
        pltpu.make_async_copy(z, both.at[pl.ds(cut, cut), :], sems.at[1]),
    ]
    for copy in copies:
        copy.start()
    core = lax.axis_index("dp") % CORES

    @pl.when(core == 0)
    def _():
        run([pltpu.make_async_copy(z, send, sems.at[2])])

    @pl.when(core != 0)
    def _():
        run([pltpu.make_async_copy(y, send, sems.at[2])])

    for copy in copies:
        copy.wait()


def join_kernel(a, b, both, sems):
    cut = a.shape[0]
    run(
        [
            pltpu.make_async_copy(a, both.at[pl.ds(0, cut), :], sems.at[0]),
            pltpu.make_async_copy(b, both.at[pl.ds(cut, cut), :], sems.at[1]),
        ]
    )


def on_device(features, centers, targets):
    n_dp, n_center = lax.axis_size("dp"), lax.axis_size("center")
    chips, halves = n_dp // CORES, n_center // QUAD
    dp_at, center_at = lax.axis_index("dp"), lax.axis_index("center")
    core, quad = dp_at % CORES, center_at % QUAD
    examples, columns, block = features.shape[0], targets.shape[1], centers.shape[0]
    total_rows = examples * n_dp
    w = columns // (QUAD * CORES)
    half = block // CORES

    def swap(value):
        return lax.ppermute(value, "dp", [(i, i ^ 1) for i in range(n_dp)])

    def over_quad(value, hop):
        return lax.ppermute(value, "center", [(j, j ^ hop) for j in range(n_center)])

    def others(value, axis, size, inner):
        n = size * inner
        got = None
        for shift in range(1, size):
            pairs = [(i, (i // inner + shift) % size * inner + i % inner) for i in range(n)]
            piece = lax.ppermute(value, axis, pairs)
            got = piece if got is None else got.astype(F32) + piece.astype(F32)
        return got

    def over_x(value):
        return others(value, "dp", chips, CORES)

    def over_halves(value):
        return others(value, "center", halves, QUAD)

    sd = jax.ShapeDtypeStruct
    place = jnp.stack([core, quad]).astype(jnp.int32)
    depth = centers.shape[1]
    mine_size = half * depth
    any_space = pl.BlockSpec(memory_space=pl.ANY)
    cut = half // CHUNKS
    chunks = vmem_call(
        split_kernel,
        [sd((cut, depth), BF16)] * CHUNKS,
        [pltpu.SemaphoreType.DMA((CHUNKS,))],
        flops=1000000,
        limit=(64 << 20) - 2 * (mine_size + targets.size) - (1 << 19),
        in_specs=[any_space],
    )(centers)
    y_in, z_in = [], []
    for k in range(CHUNKS):
        y_in.append(over_quad(chunks[k], 1))
        z_in.append(over_quad(chunks[k], 2))
    features_two = swap(features)
    features_two, = vmem_call(
        keep_kernel,
        [pltpu.VMEM(features.shape, BF16)],
        [pltpu.SemaphoreType.DMA(())],
        flops=1000000,
        in_specs=[any_space],
    )(features_two)

    row = lax.broadcasted_iota(jnp.int32, (CORES * QUAD * w, columns), 0)
    group = (quad ^ (row // w % QUAD)) * CORES + (core ^ (row // (QUAD * w)))
    chosen = (group * w + row % w == lax.broadcasted_iota(jnp.int32, row.shape, 1)).astype(BF16)
    wanted = lax.dot_general(chosen, targets, NT, preferred_element_type=F32).astype(BF16)
    wanted_two = swap(wanted[QUAD * w :])
    wanted = wanted[: QUAD * w]

    def build(rows):
        return kernel_block(features, rows), kernel_block(features_two, rows)

    own = build(centers)
    wide = QUAD * block
    flops = 2 * 256 * CORES * examples * wide
    side, = vmem_call(side_kernel, [sd((QUAD * w, block), F32)], flops=flops // 4)(
        wanted, wanted_two, *own
    )
    got_side = over_x(side)
    pairs = []
    for i in range(n_dp):
        hop = 1 if i % CORES == 0 else 2
        pairs += [(i * n_center + j, i * n_center + (j ^ hop)) for j in range(n_center)]
    early_groups, d_in = [own], []
    for k in range(CHUNKS):
        near, d_send = vmem_call(
            fork_kernel,
            [pltpu.VMEM((2 * cut, depth), BF16), pltpu.VMEM((cut, depth), BF16)],
            [pltpu.SemaphoreType.DMA((3,))],
            flops=1000000,
            in_specs=[any_space] * 2,
        )(y_in[k], z_in[k])
        d_in.append(lax.ppermute(d_send, ("dp", "center"), pairs))
        far = swap(near)
        early_groups.append(build(near))
        early_groups.append(build(far))
    sides = vmem_call(
        functools.partial(right_kernel, 1.0 / math.sqrt(total_rows)), [sd((w, block), F32)] * QUAD, flops=1000000
    )(side, got_side)
    sides = [sides[0]] + [over_quad(sides[hop], hop) for hop in range(1, QUAD)]
    early_pieces = [p[0] for p in early_groups]
    d_near = d_in[0]
    if CHUNKS > 1:
        d_near, = vmem_call(
            join_kernel,
            [pltpu.VMEM((half, depth), BF16)],
            [pltpu.SemaphoreType.DMA((CHUNKS,))],
            flops=1000000,
            in_specs=[any_space] * CHUNKS,
        )(*d_in)
    d_far = swap(d_near)
    d_0, d_1 = build(d_near), build(d_far)
    late_pieces = [d_0[0], d_1[0]]
    part = sd((w, examples), F32), sd((w, examples), BF16)
    right_side, low_last, early = vmem_call(
        functools.partial(early_kernel, len(early_pieces), wide - block),
        [sd((w, wide), F32), sd((w, block), BF16), part[0]],
        flops=flops * 3 // 8,
    )(*sides, *early_pieces)
    one = early_pieces + late_pieces
    two = [p[1] for p in early_groups] + [d_0[1], d_1[1]]
    partial, low = vmem_call(late_kernel, part, flops=flops // 8)(low_last, early, *late_pieces)
    got = over_halves(low)
    partial_two, low_two = vmem_call(second_kernel, part, flops=flops // 2)(right_side, *two)
    got_two = over_halves(low_two)
    image_shape, sums_shape = sd((w, wide), F32), sd((w, LANES), F32)
    image, _ = vmem_call(back_kernel, [image_shape, sums_shape], flops=flops // 2)(partial, got, *one)
    image, = vmem_call(back_rest_kernel, [image_shape], flops=flops // 2)(partial_two, got_two, image, *two)
    got = over_x(image)
    image, dots = vmem_call(functools.partial(sums_kernel, total_rows), [image_shape, sums_shape], flops=1000000)(
        image, got, right_side
    )
    got_dots = over_halves(dots)
    residual, direction, partial, low = vmem_call(
        middle_kernel, [image_shape, image_shape, *part], flops=flops // 2
    )(dots, got_dots, right_side, image, *one)
    got = over_halves(low)
    partial_two, low_two = vmem_call(second_kernel, part, flops=flops // 2)(direction, *two)
    got_two = over_halves(low_two)
    image, squares = vmem_call(back_kernel, [image_shape, sums_shape], flops=flops // 2)(partial, got, *one)
    image, image_low = vmem_call(
        back_last_kernel, [image_shape, sd((w, wide + LANES), BF16)], flops=flops // 2
    )(partial_two, got_two, image, squares, *two)
    got = over_x(image_low)
    finals = vmem_call(
        functools.partial(last_kernel, total_rows), [sd((2 * w, block), BF16)] * QUAD, flops=1000000
    )(dots, got_dots, image_low, image, got, right_side, residual, direction)
    landed = [finals[0]]
    for hop in range(1, QUAD):
        landed.append(over_quad(finals[hop], hop))
    landed_two = [swap(piece) for piece in landed]
    return tuple(
        vmem_call(
            functools.partial(place_kernel, w),
            [sd((block, columns), F32)] * 2,
            [pltpu.VMEM((columns, block), BF16)] * 2,
            flops=1000000,
            in_specs=[pl.BlockSpec(memory_space=pltpu.SMEM)] + [pl.BlockSpec(memory_space=pltpu.VMEM)] * (2 * QUAD),
        )(place, *landed, *landed_two)
    )


def solution(mesh):
    placed = (P("dp", None), P("center", None), P("dp", None))
    return jax.shard_map(
        on_device,
        mesh=mesh,
        in_specs=placed,
        out_specs=(P("center", None), P("center", None)),
        check_vma=False,
    )
```

```python
import functools
import math

import jax
import jax.numpy as jnp
from jax import lax
from jax.experimental import pallas as pl
from jax.experimental.pallas import tpu as pltpu
from jax.sharding import PartitionSpec as P


F32 = jnp.float32
BF16 = jnp.bfloat16
NT = (((1,), (1,)), ((), ()))
NN = (((1,), (0,)), ((), ()))
QUAD = 4
CORES = 2
TILE = 256
CHUNKS = 2
LANES = 128
WORDS = 3


def vmem_call(body, outs, scratch=(), flops=0, nbytes=0, limit=32 << 20, **kw):
    many = isinstance(outs, (list, tuple))
    return pl.pallas_call(
        body,
        out_shape=outs,
        scratch_shapes=list(scratch),
        out_specs=jax.tree.map(lambda _: pl.BlockSpec(memory_space=pltpu.VMEM), tuple(outs) if many else outs),
        compiler_params=pltpu.CompilerParams(vmem_limit_bytes=limit),
        cost_estimate=pl.CostEstimate(flops=flops, bytes_accessed=nbytes, transcendentals=0),
        **kw,
    )


def kernel_block(rows, centers):
    scores = lax.dot_general(rows, centers, NT, preferred_element_type=F32)
    lifted = 1.0 + 0.5 / math.sqrt(rows.shape[1]) * scores
    return (lifted * lifted * lifted).astype(BF16)


def times_kernel(low, refs, emit):
    for at in range(0, refs[0].shape[0], TILE):
        total, first = None, 0
        for ref in refs:
            width = ref.shape[1]
            term = lax.dot_general(
                ref[at : at + TILE, :], low[:, first : first + width], NT, preferred_element_type=F32
            )
            total = term if total is None else total + term
            first += width
        emit(slice(at, at + TILE), total.T)


def times_transposed(low, refs, store):
    first = 0
    for ref in refs:
        value = lax.dot_general(low, ref[...], NN, preferred_element_type=F32)
        store(slice(first, first + ref.shape[1]), value)
        first += ref.shape[1]


def side_kernel(first, second, one, two, out):
    out[...] = lax.dot_general(first[...], one[...], NN, preferred_element_type=F32)
    out[...] += lax.dot_general(second[...], two[...], NN, preferred_element_type=F32)


def right_kernel(scale, own, got, *out):
    w = out[0].shape[0]
    for hop in range(QUAD):
        rows = slice(hop * w, (hop + 1) * w)
        out[hop][...] = (own[rows, :] + got[rows, :]) * scale


def segments():
    found = []
    for chunk in range(CHUNKS):
        for far in range(CORES):
            found += [(1, far, chunk), (2, far, chunk)]
    for far in range(CORES):
        found += [(3, far, chunk) for chunk in range(CHUNKS)]
    return found


def early_kernel(count, n_early, *refs):
    sides, k_refs = refs[:QUAD], refs[QUAD : QUAD + count]
    right_side, low_last, partial = refs[QUAD + count :]
    core = lax.axis_index("dp") % CORES
    width = sides[0].shape[1]
    half = width // CORES
    cut = half // CHUNKS
    right_side[:, :width] = sides[0][...]
    for index, (hop, far, chunk) in enumerate(segments()):
        at = pl.multiple_of(jnp.bitwise_xor(core, far) * half + chunk * cut, cut)
        to = width + index * cut
        right_side[:, to : to + cut] = sides[hop][:, pl.ds(at, cut)]
    low_last[...] = right_side[:, n_early:].astype(BF16)

    def emit(cols, value):
        partial[:, cols] = value

    times_kernel(right_side[:, :n_early].astype(BF16), k_refs, emit)


def late_kernel(low, early, *refs):
    k_refs, (partial, partial_low) = refs[:-2], refs[-2:]

    def emit(cols, value):
        value = value + early[:, cols]
        partial[:, cols] = value
        partial_low[:, cols] = value.astype(BF16)

    times_kernel(low, k_refs, emit)


def second_kernel(direction, *refs):
    k_refs, (partial, partial_low) = refs[:-2], refs[-2:]

    def emit(cols, value):
        partial[:, cols] = value
        partial_low[:, cols] = value.astype(BF16)

    times_kernel(direction[...].astype(BF16), k_refs, emit)


def rounded(partial, got):
    total = partial[...] + got[...].astype(F32)
    low = total.astype(BF16)
    return low, jnp.sum(total * low.astype(F32), axis=1, keepdims=True)


def back_kernel(partial, got, *refs):
    k_refs, (image, squares) = refs[:-2], refs[-2:]
    low, sums = rounded(partial, got)
    squares[...] = jnp.broadcast_to(sums, squares.shape)

    def store(cols, value):
        image[:, cols] = value

    times_transposed(low, k_refs, store)


def back_rest_kernel(partial, got, before, *refs):
    k_refs, image = refs[:-1], refs[-1]
    low, _ = rounded(partial, got)

    def store(cols, value):
        image[:, cols] = before[:, cols] + value

    times_transposed(low, k_refs, store)


def back_last_kernel(partial, got, before, squares, *refs):
    k_refs, (image, image_low) = refs[:-2], refs[-2:]
    low, left = rounded(partial, got)
    left = left + squares[:, :1]
    tail = image_low.shape[1] - LANES
    lane = lax.broadcasted_iota(jnp.int32, (left.shape[0], LANES), 1)
    words = jnp.zeros(lane.shape, F32)
    for index in range(WORDS):
        word = left.astype(BF16).astype(F32)
        words = jnp.where(lane == index, word, words)
        left = left - word
    image_low[:, tail:] = words.astype(BF16)

    def store(cols, value):
        value = before[:, cols] + value
        image[:, cols] = value
        image_low[:, cols] = value.astype(BF16)

    times_transposed(low, k_refs, store)


def sums_kernel(rows, own, got, right_side, image, sums):
    direction = right_side[...]
    value = (own[...] + got[...]) * (1.0 / rows) + 0.5 * direction
    image[...] = value
    lane = lax.broadcasted_iota(jnp.int32, sums.shape, 1)
    found = jnp.zeros(sums.shape, F32)
    for index, product in enumerate((direction * direction, direction * value, value * value)):
        found = jnp.where(lane == index, jnp.sum(product, axis=1, keepdims=True), found)
    sums[...] = found


def scalars(own_sums, got_sums):
    total = own_sums[...] + got_sums[...]
    norm, curvature, image_sq = [total[:, k : k + 1] for k in range(3)]
    step = norm / (curvature + 1e-06)
    norm_next = norm - 2.0 * step * curvature + step * step * image_sq
    ratio = norm_next / (norm + 1e-06)
    direction_sq = norm_next + 2.0 * ratio * (norm - step * curvature) + ratio * ratio * norm
    return step, norm_next, ratio, direction_sq


def middle_kernel(own_sums, got_sums, right_side, image, *refs):
    k_refs, (residual, direction, partial, partial_low) = refs[:-4], refs[-4:]
    step, _, ratio, _ = scalars(own_sums, got_sums)
    first = right_side[...]
    res = first - step * image[...]
    new = res + ratio * first
    residual[...] = res
    direction[...] = new

    def emit(cols, value):
        partial[:, cols] = value
        partial_low[:, cols] = value.astype(BF16)

    times_kernel(new.astype(BF16), k_refs, emit)


def last_kernel(rows, own_sums, got_sums, low, own, got, right_side, residual, direction, *out):
    step, norm_next, _, direction_sq = scalars(own_sums, got_sums)
    wide = own.shape[1]
    squares = low[:, wide:].astype(F32) + got[:, wide:].astype(F32)
    curvature = jnp.sum(squares, axis=1, keepdims=True) * (1.0 / rows) + 0.5 * direction_sq
    step_two = norm_next / (curvature + 1e-06)
    new = direction[...]
    image = (own[...] + got[:, :wide].astype(F32)) * (1.0 / rows) + 0.5 * new
    coef = (step * right_side[...] + step_two * new).astype(BF16)
    res = (residual[...] - step_two * image).astype(BF16)
    w = coef.shape[0]
    width = out[0].shape[1]
    half = width // CORES
    cut = half // CHUNKS
    for first, value in ((0, coef), (w, res)):
        rows = slice(first, first + w)
        out[0][rows, :] = value[:, :width]
        for index, (hop, far, chunk) in enumerate(segments()):
            at, to = width + index * cut, far * half + chunk * cut
            out[hop][rows, to : to + cut] = value[:, at : at + cut]


def place_kernel(w, *refs):
    mine, other = refs[:QUAD], refs[QUAD : 2 * QUAD]
    coef, residual, coef_t, residual_t = refs[2 * QUAD :]
    core, quad = lax.axis_index("dp") % CORES, lax.axis_index("center") % QUAD
    half = coef.shape[0] // CORES
    for hop in range(QUAD):
        group = jnp.bitwise_xor(quad, hop) * CORES
        for swapped, piece, at in ((0, mine[hop], group + core), (1, other[hop], group + 1 - core)):
            rows = pl.ds(pl.multiple_of(at * w, w), w)
            for index in range(CORES):
                to = index if hop == 0 else jnp.bitwise_xor(core, index ^ swapped)
                cols = pl.ds(pl.multiple_of(to * half, half), half)
                source = slice(index * half, (index + 1) * half)
                coef_t[rows, cols] = piece[0:w, source]
                residual_t[rows, cols] = piece[w : 2 * w, source]
    coef[...] = coef_t[...].T.astype(F32)
    residual[...] = residual_t[...].T.astype(F32)


def run(copies):
    for copy in copies:
        copy.start()
    for copy in copies:
        copy.wait()


def split_kernel(centers, *refs):
    chunks, sems = refs[:-1], refs[-1]
    cut = chunks[0].shape[0]
    at = (lax.axis_index("dp") % CORES) * (cut * CHUNKS)
    run(
        [
            pltpu.make_async_copy(centers.at[pl.ds(pl.multiple_of(at + k * cut, cut), cut), :], chunk, sems.at[k])
            for k, chunk in enumerate(chunks)
        ]
    )


def keep_kernel(value, out, sem):
    run([pltpu.make_async_copy(value, out, sem)])


def fork_kernel(y, z, both, send, sems):
    cut = y.shape[0]
    copies = [
        pltpu.make_async_copy(y, both.at[pl.ds(0, cut), :], sems.at[0]),
        pltpu.make_async_copy(z, both.at[pl.ds(cut, cut), :], sems.at[1]),
    ]
    for copy in copies:
        copy.start()
    core = lax.axis_index("dp") % CORES

    @pl.when(core == 0)
    def _():
        run([pltpu.make_async_copy(z, send, sems.at[2])])

    @pl.when(core != 0)
    def _():
        run([pltpu.make_async_copy(y, send, sems.at[2])])

    for copy in copies:
        copy.wait()


def join_kernel(a, b, both, sems):
    cut = a.shape[0]
    run(
        [
            pltpu.make_async_copy(a, both.at[pl.ds(0, cut), :], sems.at[0]),
            pltpu.make_async_copy(b, both.at[pl.ds(cut, cut), :], sems.at[1]),
        ]
    )


def on_device(features, centers, targets):
    n_dp, n_center = lax.axis_size("dp"), lax.axis_size("center")
    chips, halves = n_dp // CORES, n_center // QUAD
    dp_at, center_at = lax.axis_index("dp"), lax.axis_index("center")
    core, quad = dp_at % CORES, center_at % QUAD
    examples, columns, block = features.shape[0], targets.shape[1], centers.shape[0]
    total_rows = examples * n_dp
    w = columns // (QUAD * CORES)
    half = block // CORES

    def swap(value):
        return lax.ppermute(value, "dp", [(i, i ^ 1) for i in range(n_dp)])

    def over_quad(value, hop):
        return lax.ppermute(value, "center", [(j, j ^ hop) for j in range(n_center)])

    def others(value, axis, size, inner):
        n = size * inner
        got = None
        for shift in range(1, size):
            pairs = [(i, (i // inner + shift) % size * inner + i % inner) for i in range(n)]
            piece = lax.ppermute(value, axis, pairs)
            got = piece if got is None else got.astype(F32) + piece.astype(F32)
        return got

    def over_x(value):
        return others(value, "dp", chips, CORES)

    def over_halves(value):
        return others(value, "center", halves, QUAD)

    sd = jax.ShapeDtypeStruct
    depth = centers.shape[1]
    any_space = pl.BlockSpec(memory_space=pl.ANY)
    cut = half // CHUNKS
    chunks = vmem_call(
        split_kernel,
        [sd((cut, depth), BF16)] * CHUNKS,
        [pltpu.SemaphoreType.DMA((CHUNKS,))],
        flops=1000000,
        limit=(64 << 20) - 2 * (half * depth + targets.size) - (1 << 19),
        in_specs=[any_space],
    )(centers)
    y_in, z_in = [], []
    for k in range(CHUNKS):
        y_in.append(over_quad(chunks[k], 1))
        z_in.append(over_quad(chunks[k], 2))
    features_two = swap(features)
    features_two, = vmem_call(
        keep_kernel,
        [pltpu.VMEM(features.shape, BF16)],
        [pltpu.SemaphoreType.DMA(())],
        flops=1000000,
        in_specs=[any_space],
    )(features_two)

    row = lax.broadcasted_iota(jnp.int32, (CORES * QUAD * w, columns), 0)
    group = (quad ^ (row // w % QUAD)) * CORES + (core ^ (row // (QUAD * w)))
    chosen = (group * w + row % w == lax.broadcasted_iota(jnp.int32, row.shape, 1)).astype(BF16)
    wanted = lax.dot_general(chosen, targets, NT, preferred_element_type=F32).astype(BF16)
    wanted_two = swap(wanted[QUAD * w :])
    wanted = wanted[: QUAD * w]

    def build(rows):
        return kernel_block(features, rows), kernel_block(features_two, rows)

    own = build(centers)
    wide = QUAD * block
    flops = 2 * 256 * CORES * examples * wide
    side, = vmem_call(side_kernel, [sd((QUAD * w, block), F32)], flops=flops // 4)(
        wanted, wanted_two, *own
    )
    got_side = over_x(side)
    pairs = []
    for i in range(n_dp):
        hop = 1 if i % CORES == 0 else 2
        pairs += [(i * n_center + j, i * n_center + (j ^ hop)) for j in range(n_center)]
    early_groups, d_in = [own], []
    for k in range(CHUNKS):
        near, d_send = vmem_call(
            fork_kernel,
            [pltpu.VMEM((2 * cut, depth), BF16), pltpu.VMEM((cut, depth), BF16)],
            [pltpu.SemaphoreType.DMA((3,))],
            flops=1000000,
            in_specs=[any_space] * 2,
        )(y_in[k], z_in[k])
        d_in.append(lax.ppermute(d_send, ("dp", "center"), pairs))
        far = swap(near)
        early_groups.append(build(near))
        early_groups.append(build(far))
    sides = vmem_call(
        functools.partial(right_kernel, 1.0 / math.sqrt(total_rows)), [sd((w, block), F32)] * QUAD, flops=1000000
    )(side, got_side)
    sides = [sides[0]] + [over_quad(sides[hop], hop) for hop in range(1, QUAD)]
    early_pieces = [p[0] for p in early_groups]
    d_near = d_in[0]
    if CHUNKS > 1:
        d_near, = vmem_call(
            join_kernel,
            [pltpu.VMEM((half, depth), BF16)],
            [pltpu.SemaphoreType.DMA((CHUNKS,))],
            flops=1000000,
            in_specs=[any_space] * CHUNKS,
        )(*d_in)
    d_far = swap(d_near)
    d_0, d_1 = build(d_near), build(d_far)
    late_pieces = [d_0[0], d_1[0]]
    part = sd((w, examples), F32), sd((w, examples), BF16)
    right_side, low_last, early = vmem_call(
        functools.partial(early_kernel, len(early_pieces), wide - block),
        [sd((w, wide), F32), sd((w, block), BF16), part[0]],
        flops=flops * 3 // 8,
    )(*sides, *early_pieces)
    one = early_pieces + late_pieces
    two = [p[1] for p in early_groups] + [d_0[1], d_1[1]]
    partial, low = vmem_call(late_kernel, part, flops=flops // 8)(low_last, early, *late_pieces)
    got = over_halves(low)
    partial_two, low_two = vmem_call(second_kernel, part, flops=flops // 2)(right_side, *two)
    got_two = over_halves(low_two)
    image_shape, sums_shape = sd((w, wide), F32), sd((w, LANES), F32)
    image, _ = vmem_call(back_kernel, [image_shape, sums_shape], flops=flops // 2)(partial, got, *one)
    image, = vmem_call(back_rest_kernel, [image_shape], flops=flops // 2)(partial_two, got_two, image, *two)
    got = over_x(image)
    image, dots = vmem_call(functools.partial(sums_kernel, total_rows), [image_shape, sums_shape], flops=1000000)(
        image, got, right_side
    )
    got_dots = over_halves(dots)
    residual, direction, partial, low = vmem_call(
        middle_kernel, [image_shape, image_shape, *part], flops=flops // 2
    )(dots, got_dots, right_side, image, *one)
    got = over_halves(low)
    partial_two, low_two = vmem_call(second_kernel, part, flops=flops // 2)(direction, *two)
    got_two = over_halves(low_two)
    image, squares = vmem_call(back_kernel, [image_shape, sums_shape], flops=flops // 2)(partial, got, *one)
    image, image_low = vmem_call(
        back_last_kernel, [image_shape, sd((w, wide + LANES), BF16)], flops=flops // 2
    )(partial_two, got_two, image, squares, *two)
    got = over_x(image_low)
    finals = vmem_call(
        functools.partial(last_kernel, total_rows), [sd((2 * w, block), BF16)] * QUAD, flops=1000000
    )(dots, got_dots, image_low, image, got, right_side, residual, direction)
    landed = [finals[0]]
    for hop in range(1, QUAD):
        landed.append(over_quad(finals[hop], hop))
    landed_two = [swap(piece) for piece in landed]
    return tuple(
        vmem_call(
            functools.partial(place_kernel, w),
            [sd((block, columns), F32)] * 2,
            [pltpu.VMEM((columns, block), BF16)] * 2,
            flops=1000000,
        )(*landed, *landed_two)
    )


def solution(mesh):
    placed = (P("dp", None), P("center", None), P("dp", None))
    return jax.shard_map(
        on_device,
        mesh=mesh,
        in_specs=placed,
        out_specs=(P("center", None), P("center", None)),
        check_vma=False,
    )
```
